32 devices in a mesh: prow: 4 (over y, core), pcol: 8 (over z, x).
Axes of the slice: x: 2, y: 2, z: 4, core: 2. Of those that a mesh axis runs over, the one named last changes fastest.
Arguments:
- matrix: bfloat16 [2, 8, 4, 256, 2, 8, 256], P(None, None, 'prow', None, None, 'pcol'), may hold values from -6 to 6
Outputs:
- image: float32 [2, 8, 4, 256, 2, 8, 256], P(None, None, 'prow', None, None, 'pcol')
The draws below stay inside these ranges and needn't reach their ends.
All inputs are finite; a program needn't handle non-finite values.
Results may differ from the reference program's by a relative error of at most 0.0003.
Values sent between devices are 32-bit elements; how exact they have to be, the bound alone decides.
A program may use at most 64 MiB of HBM per device.

```python
import jax
import jax.numpy as jnp

IMAGES = 2
BLOCK = 256
ROW_BLOCKS = 8
COL_BLOCKS = 2
N_PROW = 4
N_PCOL = 8


def block_levels(key, extent, shards, low, high):
    loudness, own = 1.0, jax.random.fold_in(key, 6)
    for position, parts in shards:
        heights = jnp.exp(jax.random.uniform(jax.random.fold_in(own, position), (parts,), jnp.float32, low / len(shards), high / len(shards)))
        loudness = loudness * jnp.repeat(heights, extent[position] // parts).reshape([-1 if axis == position else 1 for axis in range(len(extent))])
    return loudness


def normal_values(stream_key, extent, spread, bound, split=(), kind=jnp.bfloat16):
    factor_of = block_levels(stream_key, extent, split, -0.22, 0.18) if split else 1.0
    result = jax.random.normal(stream_key, extent, jnp.float32) * spread * factor_of
    return jnp.minimum(jnp.maximum(result, -bound), bound).astype(kind)


def setup_inputs(seed: int = 0) -> dict:
    arg_keys = jax.random.split(jax.random.key(seed), 2)
    matrix = normal_values(arg_keys[0], (IMAGES, ROW_BLOCKS, N_PROW, BLOCK, COL_BLOCKS, N_PCOL, BLOCK), 1.0, 6.0, ((2, 4), (5, 8)))
    return {"matrix": matrix}


def reference(matrix):
    total_rows = ROW_BLOCKS * N_PROW * BLOCK
    total_cols = COL_BLOCKS * N_PCOL * BLOCK
    full = matrix.astype(jnp.float32).reshape(IMAGES, total_rows, total_cols)
    summed = jnp.cumsum(jnp.cumsum(full, axis=1, dtype=jnp.float32), axis=2, dtype=jnp.float32)
    row_factor = 1.0 / jnp.sqrt(jnp.arange(total_rows).astype(jnp.float32) + 1.0)
    col_factor = 1.0 / jnp.sqrt(jnp.arange(total_cols).astype(jnp.float32) + 1.0)
    scaled = summed * (row_factor[None, :, None] * col_factor[None, None, :])
    return scaled.reshape(IMAGES, ROW_BLOCKS, N_PROW, BLOCK, COL_BLOCKS, N_PCOL, BLOCK)
```

```python
import functools

import jax
import jax.numpy as jnp
from jax import lax
from jax.experimental import pallas as pl
from jax.experimental.pallas import tpu as pltpu
from jax.sharding import PartitionSpec as P

F32, BF16 = jnp.float32, jnp.bfloat16
HIGH = lax.Precision.HIGHEST
MESH = pl.DeviceIdType.MESH
NN = (((1,), (0,)), ((), ()))
NT = (((1,), (1,)), ((), ()))


def iotas(rows, cols):
    return (lax.broadcasted_iota(jnp.int32, (rows, cols), 0), lax.broadcasted_iota(jnp.int32, (rows, cols), 1))


def dot(a, b, dims=NN, precision=None):
    return lax.dot_general(a, b, dims, precision=precision, preferred_element_type=F32)


def split3(x):
    hi = x.astype(BF16)
    rest = x - hi.astype(F32)
    mid = rest.astype(BF16)
    return hi, mid, (rest - mid.astype(F32)).astype(BF16)


def carries(np_, nq, rows_here, x_hbm, cum_ref, d_ref, xbuf, rs_loc, cs_loc, t_loc, rs_all, cs_all, t_all,
            in_sem, rs_send, rs_recv, cs_send, cs_recv, t_send, t_recv):
    groups, tile, cols, width = x_hbm.shape
    merged = tile * cols
    p, q = lax.axis_index("prow"), lax.axis_index("pcol")
    total = np_ * nq
    me = p * nq + q
    loads = [pltpu.make_async_copy(x_hbm.at[g], xbuf.at[g], in_sem.at[g]) for g in range(groups)]
    for load in loads:
        load.start()

    barrier = pltpu.get_barrier_semaphore()

    def greet(k, _):
        dev = lax.rem(me + k, total)
        pl.semaphore_signal(barrier, inc=1, device_id=(dev // nq, lax.rem(dev, nq)), device_id_type=MESH)
        return 0

    lax.fori_loop(1, total, greet, 0)

    row_g, _ = iotas(groups, width)
    pick_r, pick_l = iotas(groups * cols, merged)
    rs = jnp.zeros((groups, merged), F32)
    cs = jnp.zeros((groups * cols, width), F32)
    for g in range(groups):
        loads[g].wait()
        x = xbuf[g].reshape(merged, width)
        rs = rs + dot((row_g == g).astype(BF16), x, NT)
        cs = cs + dot((pick_r == g * cols + lax.rem(pick_l, cols)).astype(BF16), x)
    rs_loc[...] = rs
    cs_loc[...] = cs
    t_loc[0] = dot(jnp.ones((8, width), F32), jnp.concatenate(
        [cs, jnp.zeros((128 - groups * cols, width), F32)], axis=0), NT, HIGH)[0:1]
    pl.semaphore_wait(barrier, total - 1)

    def rs_copy(k, sender, target):
        return pltpu.make_async_remote_copy(
            src_ref=rs_loc, dst_ref=rs_all.at[sender], send_sem=rs_send.at[k], recv_sem=rs_recv.at[sender],
            device_id=(p, target), device_id_type=MESH)

    def cs_copy(k, sender, target):
        return pltpu.make_async_remote_copy(
            src_ref=cs_loc, dst_ref=cs_all.at[sender], send_sem=cs_send.at[k], recv_sem=cs_recv.at[sender],
            device_id=(target, q), device_id_type=MESH)

    def t_copy(k, sender, target):
        return pltpu.make_async_remote_copy(
            src_ref=t_loc.at[0], dst_ref=t_all.at[sender], send_sem=t_send.at[k], recv_sem=t_recv.at[sender],
            device_id=(target // nq, lax.rem(target, nq)), device_id_type=MESH)

    kinds = ((t_copy, me, total), (cs_copy, p, np_), (rs_copy, q, nq))
    for make, here, count in kinds:
        def send(k, _):
            make(k, here, lax.rem(here + k, count)).start()
            return 0
        lax.fori_loop(1, count, send, 0)

    def drain(make, here, count):
        def wait(k, _):
            make(k, lax.rem(here + k, count), lax.rem(here + k, count)).wait_recv()
            return 0
        lax.fori_loop(1, count, wait, 0)

    drain(*kinds[0])
    t_all[pl.ds(me, 1)] = t_loc[...]

    def t_sum(k, acc):
        a_all, a_lt, b_all, b_lt = acc
        value = t_all[k]
        kp, kq = k // nq, lax.rem(k, nq)
        left = jnp.where(kq < q, value, 0.0)
        up = jnp.where(kp < p, value, 0.0)
        both = jnp.where(kp < p, left, 0.0)
        return a_all + left, a_lt + both, b_all + value, b_lt + up

    zero = jnp.zeros((1, 128), F32)
    a_all, a_lt, b_all, b_lt = lax.fori_loop(0, total, t_sum, (zero,) * 4)
    out, src = iotas(groups * cols, 128)
    out_g, src_g = out // cols, src // cols
    out_c, src_c = lax.rem(out, cols), lax.rem(src, cols)
    same_g = out_g == src_g
    above = (out_g // rows_here == src_g // rows_here) & (src_g < out_g)

    def pair(strict, equal, all_rows, lt_rows):
        wide = jnp.concatenate([jnp.where(above & strict, 1.0, 0.0), jnp.where(same_g & strict, 1.0, 0.0)], axis=1)
        return jnp.sum(wide * jnp.concatenate([all_rows, lt_rows], axis=1), axis=1, keepdims=True)

    corner = pair(src_c == out_c, None, a_all, a_lt) + pair(src_c < out_c, None, b_all, b_lt)

    drain(*kinds[1])
    c_all, c_lt = cs, jnp.zeros_like(cs)
    for k in range(np_):
        value = jnp.where(k == p, 0.0, cs_all[k])
        c_all = c_all + value
        c_lt = c_lt + jnp.where(k < p, value, 0.0)
    o, s = iotas(groups * cols, groups * cols)
    strict = ((o // (rows_here * cols) == s // (rows_here * cols)) & (lax.rem(o, cols) == lax.rem(s, cols))
              & (s // cols < o // cols)).astype(F32)
    pre = dot(strict, c_all, NN, HIGH) + c_lt
    u0, u1 = iotas(width, width)
    d_ref[...] = dot(pre, (u0 <= u1).astype(F32), NN, HIGH) + corner

    i0, i1 = iotas(merged, merged)
    reach = i1 // cols <= i0 // cols
    c0, c1 = lax.rem(i0, cols), lax.rem(i1, cols)
    low = (reach & (c0 == c1)).astype(BF16)
    low_all = (reach & (c1 < c0)).astype(BF16)
    drain(*kinds[2])
    r_all, r_lt = rs, jnp.zeros_like(rs)
    for k in range(nq):
        value = jnp.where(k == q, 0.0, rs_all[k])
        r_all = r_all + value
        r_lt = r_lt + jnp.where(k < q, value, 0.0)
    cum = jnp.zeros((merged, groups), F32)
    for part_lt, part_all in zip(split3(r_lt), split3(r_all)):
        cum = cum + dot(low, part_lt, NT) + dot(low_all, part_all, NT)
    parts = split3(cum)
    cum_ref[...] = jnp.concatenate(
        [*(part.astype(F32) for part in parts), jnp.zeros((merged, 128 - 3 * groups), F32)], axis=1).astype(BF16)

    for make, here, count in kinds:
        def sent(k, _):
            make(k, here, lax.rem(here + k, count)).wait_send()
            return 0
        lax.fori_loop(1, count, sent, 0)


def finish(np_, nq, rows_here, groups, x_ref, cum_ref, d_ref, o_ref, low_ref, up_ref, cf_ref):
    tile, cols, width = x_ref.shape
    merged = tile * cols
    g = pl.program_id(0)
    p, q = lax.axis_index("prow"), lax.axis_index("pcol")

    @pl.when(g == 0)
    def _():
        i0, i1 = iotas(merged, merged)
        low_ref[...] = ((i1 <= i0) & (lax.rem(i0 - i1 + merged, cols) == 0)).astype(BF16)
        u0, u1 = iotas(width, width)
        up_ref[...] = (u0 <= u1).astype(BF16)
        c0, c1 = iotas(8, width)
        cf_ref[...] = 1.0 / jnp.sqrt((((lax.rem(c0, cols) * nq + q) * width + c1) + 1).astype(F32))

    x = x_ref[...].reshape(merged, width)
    y = dot(low_ref[...], x)
    hi = y.astype(BF16)
    lo = (y - hi.astype(F32)).astype(BF16)
    l0, _ = iotas(128, width)
    pick = ((lax.rem(l0, groups) == g) & (l0 < 3 * groups)).astype(BF16)
    s = dot(hi, up_ref[...]) + dot(lo, up_ref[...]) + dot(cum_ref[...], pick)
    d = d_ref[...].reshape(cols, width)
    dd = jnp.concatenate([d] * (8 // cols), axis=0)
    a0, _ = iotas(merged, 128)
    rf = 1.0 / jnp.sqrt((((lax.rem(g, rows_here) * np_ + p) * tile + a0 // cols) + 1).astype(F32))
    for t in range(width // 128):
        cut = slice(t * 128, (t + 1) * 128)
        part = s[:, cut].reshape(merged // 8, 8, 128) + dd[None, :, cut]
        part = part * (rf.reshape(merged // 8, 8, 128) * cf_ref[:, cut][None])
        o_ref[pl.ds(t, merged, stride=width // 128), :] = part.reshape(merged, 128)


def solution(mesh):
    np_, nq = mesh.shape["prow"], mesh.shape["pcol"]

    def shards(matrix):
        batch, rows_here, _, tile, cols, _, width = matrix.shape
        groups, merged, lanes = batch * rows_here, tile * cols, width // 128
        x = matrix.reshape(groups, tile, cols, width)
        dma = pltpu.SemaphoreType.DMA
        vmem = pl.BlockSpec(memory_space=pltpu.VMEM)
        total = np_ * nq
        cum, d = pl.pallas_call(
            functools.partial(carries, np_, nq, rows_here),
            out_shape=(jax.ShapeDtypeStruct((merged, 128), BF16), jax.ShapeDtypeStruct((groups * cols, width), F32)),
            in_specs=[pl.BlockSpec(memory_space=pl.ANY)],
            out_specs=(vmem, vmem),
            scratch_shapes=[
                pltpu.VMEM((groups, tile, cols, width), BF16),
                pltpu.VMEM((groups, merged), F32),
                pltpu.VMEM((groups * cols, width), F32),
                pltpu.VMEM((1, 1, 128), F32),
                pltpu.VMEM((nq, groups, merged), F32),
                pltpu.VMEM((np_, groups * cols, width), F32),
                pltpu.VMEM((total, 1, 128), F32),
                dma((groups,)), dma((nq,)), dma((nq,)), dma((np_,)), dma((np_,)), dma((total,)), dma((total,)),
            ],
            compiler_params=pltpu.CompilerParams(
                collective_id=0, has_side_effects=True, vmem_limit_bytes=40 * 2**20),
            name="carries",
        )(x)
        out = pl.pallas_call(
            functools.partial(finish, np_, nq, rows_here, groups),
            grid=(groups,),
            out_shape=jax.ShapeDtypeStruct((groups, merged * lanes, 128), F32),
            in_specs=[
                pl.BlockSpec((None, tile, cols, width), lambda g: (g, 0, 0, 0)),
                pl.BlockSpec((merged, 128), lambda g: (0, 0)),
                pl.BlockSpec((None, cols, width), lambda g: (g, 0, 0)),
            ],
            out_specs=pl.BlockSpec((None, merged * lanes, 128), lambda g: (g, 0, 0)),
            scratch_shapes=[pltpu.VMEM((merged, merged), BF16), pltpu.VMEM((width, width), BF16),
                            pltpu.VMEM((8, width), F32)],
            name="finish",
        )(x, cum, d.reshape(groups, cols, width))
        return out.reshape(matrix.shape)

    spec = P(None, None, "prow", None, None, "pcol", None)
    return jax.shard_map(shards, mesh=mesh, in_specs=(spec,), out_specs=spec, check_vma=False)
```

```python
import functools

import jax
import jax.numpy as jnp
from jax import lax
from jax.experimental import pallas as pl
from jax.experimental.pallas import tpu as pltpu
from jax.sharding import PartitionSpec as P

F32, BF16 = jnp.float32, jnp.bfloat16
HIGH = lax.Precision.HIGHEST
MESH = pl.DeviceIdType.MESH
NN = (((1,), (0,)), ((), ()))
NT = (((1,), (1,)), ((), ()))


def iotas(rows, cols):
    return (lax.broadcasted_iota(jnp.int32, (rows, cols), 0), lax.broadcasted_iota(jnp.int32, (rows, cols), 1))


def dot(a, b, dims=NN, precision=None):
    return lax.dot_general(a, b, dims, precision=precision, preferred_element_type=F32)


def split3(x):
    hi = x.astype(BF16)
    rest = x - hi.astype(F32)
    mid = rest.astype(BF16)
    return hi, mid, (rest - mid.astype(F32)).astype(BF16)


def carries(np_, nq, rows_here, x_hbm, cum_ref, d_ref, xbuf, rs_loc, cs_loc, t_loc, rs_all, cs_all, t_all,
            in_sem, rs_send, rs_recv, cs_send, cs_recv, t_send, t_recv):
    groups, tile, cols, width = x_hbm.shape
    merged = tile * cols
    p, q = lax.axis_index("prow"), lax.axis_index("pcol")
    total = np_ * nq
    me = p * nq + q
    loads = [pltpu.make_async_copy(x_hbm.at[g], xbuf.at[g], in_sem.at[g]) for g in range(groups)]
    for load in loads:
        load.start()

    barrier = pltpu.get_barrier_semaphore()

    def greet(k, _):
        dev = lax.rem(me + k, total)
        pl.semaphore_signal(barrier, inc=1, device_id=(dev // nq, lax.rem(dev, nq)), device_id_type=MESH)
        return 0

    lax.fori_loop(1, total, greet, 0)

    row_g, _ = iotas(groups, width)
    pick_r, pick_l = iotas(groups * cols, merged)
    rs = jnp.zeros((groups, merged), F32)
    cs = jnp.zeros((groups * cols, width), F32)
    for g in range(groups):
        loads[g].wait()
        x = xbuf[g].reshape(merged, width)
        rs = rs + dot((row_g == g).astype(BF16), x, NT)
        cs = cs + dot((pick_r == g * cols + lax.rem(pick_l, cols)).astype(BF16), x)
    rs_loc[...] = rs
    cs_loc[...] = cs
    t_loc[0] = dot(jnp.ones((8, width), F32), jnp.concatenate(
        [cs, jnp.zeros((128 - groups * cols, width), F32)], axis=0), NT, HIGH)[0:1]
    pl.semaphore_wait(barrier, total - 1)

    def rs_copy(k, sender, target):
        return pltpu.make_async_remote_copy(
            src_ref=rs_loc, dst_ref=rs_all.at[sender], send_sem=rs_send.at[k], recv_sem=rs_recv.at[sender],
            device_id=(p, target), device_id_type=MESH)

    def cs_copy(k, sender, target):
        return pltpu.make_async_remote_copy(
            src_ref=cs_loc, dst_ref=cs_all.at[sender], send_sem=cs_send.at[k], recv_sem=cs_recv.at[sender],
            device_id=(target, q), device_id_type=MESH)

    def t_copy(k, sender, target):
        return pltpu.make_async_remote_copy(
            src_ref=t_loc.at[0], dst_ref=t_all.at[sender], send_sem=t_send.at[k], recv_sem=t_recv.at[sender],
            device_id=(target // nq, lax.rem(target, nq)), device_id_type=MESH)

    kinds = ((t_copy, me, total), (cs_copy, p, np_), (rs_copy, q, nq))
    for make, here, count in kinds[::-1]:
        def send(k, _):
            make(k, here, lax.rem(here + k, count)).start()
            return 0
        lax.fori_loop(1, count, send, 0)

    def drain(make, here, count):
        def wait(k, _):
            make(k, lax.rem(here + k, count), lax.rem(here + k, count)).wait_recv()
            return 0
        lax.fori_loop(1, count, wait, 0)

    drain(*kinds[0])
    t_all[pl.ds(me, 1)] = t_loc[...]

    def t_sum(k, acc):
        a_all, a_lt, b_all, b_lt = acc
        value = t_all[k]
        kp, kq = k // nq, lax.rem(k, nq)
        left = jnp.where(kq < q, value, 0.0)
        up = jnp.where(kp < p, value, 0.0)
        both = jnp.where(kp < p, left, 0.0)
        return a_all + left, a_lt + both, b_all + value, b_lt + up

    zero = jnp.zeros((1, 128), F32)
    a_all, a_lt, b_all, b_lt = lax.fori_loop(0, total, t_sum, (zero,) * 4)
    out, src = iotas(groups * cols, 128)
    out_g, src_g = out // cols, src // cols
    out_c, src_c = lax.rem(out, cols), lax.rem(src, cols)
    same_g = out_g == src_g
    above = (out_g // rows_here == src_g // rows_here) & (src_g < out_g)

    def pair(strict, equal, all_rows, lt_rows):
        wide = jnp.concatenate([jnp.where(above & strict, 1.0, 0.0), jnp.where(same_g & strict, 1.0, 0.0)], axis=1)
        return jnp.sum(wide * jnp.concatenate([all_rows, lt_rows], axis=1), axis=1, keepdims=True)

    corner = pair(src_c == out_c, None, a_all, a_lt) + pair(src_c < out_c, None, b_all, b_lt)

    drain(*kinds[1])
    c_all, c_lt = cs, jnp.zeros_like(cs)
    for k in range(np_):
        value = jnp.where(k == p, 0.0, cs_all[k])
        c_all = c_all + value
        c_lt = c_lt + jnp.where(k < p, value, 0.0)
    o, s = iotas(groups * cols, groups * cols)
    strict = ((o // (rows_here * cols) == s // (rows_here * cols)) & (lax.rem(o, cols) == lax.rem(s, cols))
              & (s // cols < o // cols)).astype(F32)
    pre = dot(strict, c_all, NN, HIGH) + c_lt
    u0, u1 = iotas(width, width)
    d_ref[...] = dot(pre, (u0 <= u1).astype(F32), NN, HIGH) + corner

    i0, i1 = iotas(merged, merged)
    reach = i1 // cols <= i0 // cols
    c0, c1 = lax.rem(i0, cols), lax.rem(i1, cols)
    low = (reach & (c0 == c1)).astype(BF16)
    low_all = (reach & (c1 < c0)).astype(BF16)
    drain(*kinds[2])
    r_all, r_lt = rs, jnp.zeros_like(rs)
    for k in range(nq):
        value = jnp.where(k == q, 0.0, rs_all[k])
        r_all = r_all + value
        r_lt = r_lt + jnp.where(k < q, value, 0.0)
    cum = jnp.zeros((merged, groups), F32)
    for part_lt, part_all in zip(split3(r_lt), split3(r_all)):
        cum = cum + dot(low, part_lt, NT) + dot(low_all, part_all, NT)
    parts = split3(cum)
    cum_ref[...] = jnp.concatenate(
        [*(part.astype(F32) for part in parts), jnp.zeros((merged, 128 - 3 * groups), F32)], axis=1).astype(BF16)

    for make, here, count in kinds:
        def sent(k, _):
            make(k, here, lax.rem(here + k, count)).wait_send()
            return 0
        lax.fori_loop(1, count, sent, 0)


def finish(np_, nq, rows_here, groups, x_ref, cum_ref, d_ref, o_ref, low_ref, up_ref, cf_ref):
    tile, cols, width = x_ref.shape
    merged = tile * cols
    g = pl.program_id(0)
    p, q = lax.axis_index("prow"), lax.axis_index("pcol")

    @pl.when(g == 0)
    def _():
        i0, i1 = iotas(merged, merged)
        low_ref[...] = ((i1 <= i0) & (lax.rem(i0 - i1 + merged, cols) == 0)).astype(BF16)
        u0, u1 = iotas(width, width)
        up_ref[...] = (u0 <= u1).astype(BF16)
        c0, c1 = iotas(8, width)
        cf_ref[...] = lax.rsqrt((((lax.rem(c0, cols) * nq + q) * width + c1) + 1).astype(F32))

    x = x_ref[...].reshape(merged, width)
    y = dot(low_ref[...], x)
    hi = y.astype(BF16)
    lo = (y - hi.astype(F32)).astype(BF16)
    l0, _ = iotas(128, width)
    pick = ((lax.rem(l0, groups) == g) & (l0 < 3 * groups)).astype(BF16)
    s = dot(hi, up_ref[...]) + dot(lo, up_ref[...]) + dot(cum_ref[...], pick)
    d = d_ref[...].reshape(cols, width)
    dd = jnp.concatenate([d] * (8 // cols), axis=0)
    a0, _ = iotas(merged, 128)
    rf = lax.rsqrt((((lax.rem(g, rows_here) * np_ + p) * tile + a0 // cols) + 1).astype(F32))
    for t in range(width // 128):
        cut = slice(t * 128, (t + 1) * 128)
        part = s[:, cut].reshape(merged // 8, 8, 128) + dd[None, :, cut]
        part = part * (rf.reshape(merged // 8, 8, 128) * cf_ref[:, cut][None])
        o_ref[pl.ds(t, merged, stride=width // 128), :] = part.reshape(merged, 128)


def solution(mesh):
    np_, nq = mesh.shape["prow"], mesh.shape["pcol"]

    def shards(matrix):
        batch, rows_here, _, tile, cols, _, width = matrix.shape
        groups, merged, lanes = batch * rows_here, tile * cols, width // 128
        x = matrix.reshape(groups, tile, cols, width)
        dma = pltpu.SemaphoreType.DMA
        vmem = pl.BlockSpec(memory_space=pltpu.VMEM)
        total = np_ * nq
        cum, d = pl.pallas_call(
            functools.partial(carries, np_, nq, rows_here),
            out_shape=(jax.ShapeDtypeStruct((merged, 128), BF16), jax.ShapeDtypeStruct((groups * cols, width), F32)),
            in_specs=[pl.BlockSpec(memory_space=pl.ANY)],
            out_specs=(vmem, vmem),
            scratch_shapes=[
                pltpu.VMEM((groups, tile, cols, width), BF16),
                pltpu.VMEM((groups, merged), F32),
                pltpu.VMEM((groups * cols, width), F32),
                pltpu.VMEM((1, 1, 128), F32),
                pltpu.VMEM((nq, groups, merged), F32),
                pltpu.VMEM((np_, groups * cols, width), F32),
                pltpu.VMEM((total, 1, 128), F32),
                dma((groups,)), dma((nq,)), dma((nq,)), dma((np_,)), dma((np_,)), dma((total,)), dma((total,)),
            ],
            compiler_params=pltpu.CompilerParams(
                collective_id=0, has_side_effects=True, vmem_limit_bytes=40 * 2**20),
            name="carries",
        )(x)
        out = pl.pallas_call(
            functools.partial(finish, np_, nq, rows_here, groups),
            grid=(groups,),
            out_shape=jax.ShapeDtypeStruct((groups, merged * lanes, 128), F32),
            in_specs=[
                pl.BlockSpec((None, tile, cols, width), lambda g: (g, 0, 0, 0)),
                pl.BlockSpec((merged, 128), lambda g: (0, 0)),
                pl.BlockSpec((None, cols, width), lambda g: (g, 0, 0)),
            ],
            out_specs=pl.BlockSpec((None, merged * lanes, 128), lambda g: (g, 0, 0)),
            scratch_shapes=[pltpu.VMEM((merged, merged), BF16), pltpu.VMEM((width, width), BF16),
                            pltpu.VMEM((8, width), F32)],
            name="finish",
        )(x, cum, d.reshape(groups, cols, width))
        return out.reshape(matrix.shape)

    spec = P(None, None, "prow", None, None, "pcol", None)
    return jax.shard_map(shards, mesh=mesh, in_specs=(spec,), out_specs=spec, check_vma=False)
```

```python
import functools

import jax
import jax.numpy as jnp
from jax import lax
from jax.experimental import pallas as pl
from jax.experimental.pallas import tpu as pltpu
from jax.sharding import PartitionSpec as P

F32, BF16 = jnp.float32, jnp.bfloat16
HIGH = lax.Precision.HIGHEST
MESH = pl.DeviceIdType.MESH
NN = (((1,), (0,)), ((), ()))
NT = (((1,), (1,)), ((), ()))


def iotas(rows, cols):
    return (lax.broadcasted_iota(jnp.int32, (rows, cols), 0), lax.broadcasted_iota(jnp.int32, (rows, cols), 1))


def dot(a, b, dims=NN, precision=None):
    return lax.dot_general(a, b, dims, precision=precision, preferred_element_type=F32)


def split3(x):
    hi = x.astype(BF16)
    rest = x - hi.astype(F32)
    mid = rest.astype(BF16)
    return hi, mid, (rest - mid.astype(F32)).astype(BF16)


def carries(np_, nq, rows_here, x_hbm, cum_ref, d_ref, flat_ref, xbuf, rs_loc, cs_loc, t_loc, rs_all, cs_all, t_all,
            in_sem, rs_send, rs_recv, cs_send, cs_recv, t_send, t_recv):
    groups, tile, cols, width = x_hbm.shape
    merged = tile * cols
    p, q = lax.axis_index("prow"), lax.axis_index("pcol")
    total = np_ * nq
    me = p * nq + q
    loads = [pltpu.make_async_copy(x_hbm.at[g], xbuf.at[g], in_sem.at[g]) for g in range(groups)]
    for load in loads:
        load.start()

    barrier = pltpu.get_barrier_semaphore()

    def greet(k, _):
        dev = lax.rem(me + k, total)
        pl.semaphore_signal(barrier, inc=1, device_id=(dev // nq, lax.rem(dev, nq)), device_id_type=MESH)
        return 0

    lax.fori_loop(1, total, greet, 0)

    row_g, _ = iotas(groups, width)
    pick_r, pick_l = iotas(groups * cols, merged)
    rs = jnp.zeros((groups, merged), F32)
    cs = jnp.zeros((groups * cols, width), F32)
    for g in range(groups):
        loads[g].wait()
        x = xbuf[g].reshape(merged, width)
        flat_ref[g] = x
        rs = rs + dot((row_g == g).astype(BF16), x, NT)
        cs = cs + dot((pick_r == g * cols + lax.rem(pick_l, cols)).astype(BF16), x)
    rs_loc[...] = rs
    cs_loc[...] = cs
    t_loc[0] = dot(jnp.ones((8, width), F32), jnp.concatenate(
        [cs, jnp.zeros((128 - groups * cols, width), F32)], axis=0), NT, HIGH)[0:1]
    pl.semaphore_wait(barrier, total - 1)

    def rs_copy(k, sender, target):
        return pltpu.make_async_remote_copy(
            src_ref=rs_loc, dst_ref=rs_all.at[sender], send_sem=rs_send.at[k], recv_sem=rs_recv.at[sender],
            device_id=(p, target), device_id_type=MESH)

    def cs_copy(k, sender, target):
        return pltpu.make_async_remote_copy(
            src_ref=cs_loc, dst_ref=cs_all.at[sender], send_sem=cs_send.at[k], recv_sem=cs_recv.at[sender],
            device_id=(target, q), device_id_type=MESH)

    def t_copy(k, sender, target):
        return pltpu.make_async_remote_copy(
            src_ref=t_loc.at[0], dst_ref=t_all.at[sender], send_sem=t_send.at[k], recv_sem=t_recv.at[sender],
            device_id=(target // nq, lax.rem(target, nq)), device_id_type=MESH)

    kinds = ((t_copy, me, total), (cs_copy, p, np_), (rs_copy, q, nq))
    for make, here, count in kinds:
        def send(k, _):
            make(k, here, lax.rem(here + k, count)).start()
            return 0
        lax.fori_loop(1, count, send, 0)

    def drain(make, here, count):
        def wait(k, _):
            make(k, lax.rem(here + k, count), lax.rem(here + k, count)).wait_recv()
            return 0
        lax.fori_loop(1, count, wait, 0)

    drain(*kinds[0])
    t_all[pl.ds(me, 1)] = t_loc[...]

    def t_sum(k, acc):
        a_all, a_lt, b_all, b_lt = acc
        value = t_all[k]
        kp, kq = k // nq, lax.rem(k, nq)
        left = jnp.where(kq < q, value, 0.0)
        up = jnp.where(kp < p, value, 0.0)
        both = jnp.where(kp < p, left, 0.0)
        return a_all + left, a_lt + both, b_all + value, b_lt + up

    zero = jnp.zeros((1, 128), F32)
    a_all, a_lt, b_all, b_lt = lax.fori_loop(0, total, t_sum, (zero,) * 4)
    out, src = iotas(groups * cols, 128)
    out_g, src_g = out // cols, src // cols
    out_c, src_c = lax.rem(out, cols), lax.rem(src, cols)
    same_g = out_g == src_g
    above = (out_g // rows_here == src_g // rows_here) & (src_g < out_g)

    def pair(strict, equal, all_rows, lt_rows):
        wide = jnp.concatenate([jnp.where(above & strict, 1.0, 0.0), jnp.where(same_g & strict, 1.0, 0.0)], axis=1)
        return jnp.sum(wide * jnp.concatenate([all_rows, lt_rows], axis=1), axis=1, keepdims=True)

    corner = pair(src_c == out_c, None, a_all, a_lt) + pair(src_c < out_c, None, b_all, b_lt)

    drain(*kinds[1])
    c_all, c_lt = cs, jnp.zeros_like(cs)
    for k in range(np_):
        value = jnp.where(k == p, 0.0, cs_all[k])
        c_all = c_all + value
        c_lt = c_lt + jnp.where(k < p, value, 0.0)
    o, s = iotas(groups * cols, groups * cols)
    strict = ((o // (rows_here * cols) == s // (rows_here * cols)) & (lax.rem(o, cols) == lax.rem(s, cols))
              & (s // cols < o // cols)).astype(F32)
    pre = dot(strict, c_all, NN, HIGH) + c_lt
    u0, u1 = iotas(width, width)
    d_ref[...] = (dot(pre, (u0 <= u1).astype(F32), NN, HIGH) + corner).reshape(groups, cols, width)

    i0, i1 = iotas(merged, merged)
    reach = i1 // cols <= i0 // cols
    c0, c1 = lax.rem(i0, cols), lax.rem(i1, cols)
    low = (reach & (c0 == c1)).astype(BF16)
    low_all = (reach & (c1 < c0)).astype(BF16)
    drain(*kinds[2])
    r_all, r_lt = rs, jnp.zeros_like(rs)
    for k in range(nq):
        value = jnp.where(k == q, 0.0, rs_all[k])
        r_all = r_all + value
        r_lt = r_lt + jnp.where(k < q, value, 0.0)
    cum = jnp.zeros((merged, groups), F32)
    for part_lt, part_all in zip(split3(r_lt), split3(r_all)):
        cum = cum + dot(low, part_lt, NT) + dot(low_all, part_all, NT)
    parts = split3(cum)
    cum_ref[...] = jnp.concatenate(
        [*(part.astype(F32) for part in parts), jnp.zeros((merged, 128 - 3 * groups), F32)], axis=1).astype(BF16)

    for make, here, count in kinds:
        def sent(k, _):
            make(k, here, lax.rem(here + k, count)).wait_send()
            return 0
        lax.fori_loop(1, count, sent, 0)


def finish(np_, nq, rows_here, groups, x_ref, cum_ref, d_ref, o_ref, low_ref, up_ref, cf_ref):
    merged, width = x_ref.shape
    cols = d_ref.shape[0]
    tile = merged // cols
    g = pl.program_id(0)
    p, q = lax.axis_index("prow"), lax.axis_index("pcol")

    @pl.when(g == 0)
    def _():
        i0, i1 = iotas(merged, merged)
        low_ref[...] = ((i1 <= i0) & (lax.rem(i0 - i1 + merged, cols) == 0)).astype(BF16)
        u0, u1 = iotas(width, width)
        up_ref[...] = (u0 <= u1).astype(BF16)
        c0, c1 = iotas(8, width)
        cf_ref[...] = lax.rsqrt((((lax.rem(c0, cols) * nq + q) * width + c1) + 1).astype(F32))

    x = x_ref[...]
    y = dot(low_ref[...], x)
    hi = y.astype(BF16)
    lo = (y - hi.astype(F32)).astype(BF16)
    l0, _ = iotas(128, width)
    pick = ((lax.rem(l0, groups) == g) & (l0 < 3 * groups)).astype(BF16)
    s = dot(hi, up_ref[...]) + dot(lo, up_ref[...]) + dot(cum_ref[...], pick)
    d = d_ref[...].reshape(cols, width)
    dd = jnp.concatenate([d] * (8 // cols), axis=0)
    a0, _ = iotas(merged, 128)
    rf = lax.rsqrt((((lax.rem(g, rows_here) * np_ + p) * tile + a0 // cols) + 1).astype(F32))
    for t in range(width // 128):
        cut = slice(t * 128, (t + 1) * 128)
        part = s[:, cut].reshape(merged // 8, 8, 128) + dd[None, :, cut]
        part = part * (rf.reshape(merged // 8, 8, 128) * cf_ref[:, cut][None])
        o_ref[pl.ds(t, merged, stride=width // 128), :] = part.reshape(merged, 128)


def solution(mesh):
    np_, nq = mesh.shape["prow"], mesh.shape["pcol"]

    def shards(matrix):
        batch, rows_here, _, tile, cols, _, width = matrix.shape
        groups, merged, lanes = batch * rows_here, tile * cols, width // 128
        x = matrix.reshape(groups, tile, cols, width)
        dma = pltpu.SemaphoreType.DMA
        vmem = pl.BlockSpec(memory_space=pltpu.VMEM)
        total = np_ * nq
        cum, d, flat = pl.pallas_call(
            functools.partial(carries, np_, nq, rows_here),
            out_shape=(jax.ShapeDtypeStruct((merged, 128), BF16), jax.ShapeDtypeStruct((groups, cols, width), F32),
                       jax.ShapeDtypeStruct((groups, merged, width), BF16)),
            in_specs=[pl.BlockSpec(memory_space=pl.ANY)],
            out_specs=(vmem, vmem, vmem),
            scratch_shapes=[
                pltpu.VMEM((groups, tile, cols, width), BF16),
                pltpu.VMEM((groups, merged), F32),
                pltpu.VMEM((groups * cols, width), F32),
                pltpu.VMEM((1, 1, 128), F32),
                pltpu.VMEM((nq, groups, merged), F32),
                pltpu.VMEM((np_, groups * cols, width), F32),
                pltpu.VMEM((total, 1, 128), F32),
                dma((groups,)), dma((nq,)), dma((nq,)), dma((np_,)), dma((np_,)), dma((total,)), dma((total,)),
            ],
            compiler_params=pltpu.CompilerParams(
                collective_id=0, has_side_effects=True, vmem_limit_bytes=40 * 2**20),
            name="carries",
        )(x)
        out = pl.pallas_call(
            functools.partial(finish, np_, nq, rows_here, groups),
            grid=(groups,),
            out_shape=jax.ShapeDtypeStruct((groups, merged * lanes, 128), F32),
            in_specs=[
                pl.BlockSpec((None, merged, width), lambda g: (g, 0, 0)),
                pl.BlockSpec((merged, 128), lambda g: (0, 0)),
                pl.BlockSpec((None, cols, width), lambda g: (g, 0, 0)),
            ],
            out_specs=pl.BlockSpec((None, merged * lanes, 128), lambda g: (g, 0, 0)),
            scratch_shapes=[pltpu.VMEM((merged, merged), BF16), pltpu.VMEM((width, width), BF16),
                            pltpu.VMEM((8, width), F32)],
            name="finish",
        )(flat, cum, d)
        return out.reshape(matrix.shape)

    spec = P(None, None, "prow", None, None, "pcol", None)
    return jax.shard_map(shards, mesh=mesh, in_specs=(spec,), out_specs=spec, check_vma=False)
```
